32 devices in a mesh: seq: 8 (over z, x), head: 4 (over y, core).
Axes of the slice: x: 2, y: 2, z: 4, core: 2. Of those that a mesh axis runs over, the one named last changes fastest.
Arguments:
- queries: bfloat16 [8192, 4096], P('seq', 'head'), may hold values from -8 to 8
- key_rows: bfloat16 [8192, 4096], P('seq', 'head'), may hold values from -8 to 8
- value_rows: bfloat16 [8192, 4096], P('seq', 'head'), may hold values from -6 to 6
- random_owner: int32 [128, 3], P('seq'), may hold values from 0 to 7, all different within a row; in each aligned block of 16 rows (0 to 15, 16 to 31, ...) at most 8 rows name the same one
- random_local: int32 [128, 3], P('seq'), may hold values from 0 to 15
- output_weight: bfloat16 [4096, 4096], P('head'), may hold values from -0.09375 to 0.09375
Outputs:
- layer_output: bfloat16 [8192, 4096], P(('seq', 'head'))
The draws below stay inside these ranges and needn't reach their ends.
Inputs may be any that keep to these rules, and one draw needn't show every extreme that they name: `random_owner`: each row names 3 different owners. Among the rows of one device (16 aligned rows) no owner is named more than 8 times, and in some device's rows one owner is named exactly 8 times.
All inputs are finite; a program needn't handle non-finite values.
Results may differ from the reference program's by a relative error of at most 0.0052.
Values may be sent and summed in bfloat16 or wider, within the bound.
A program may use at most 192 MiB of HBM per device.

```python
import math
import jax
import jax.numpy as jnp
import numpy as np
from jax import lax

D = 4096
HEADS = 32
HEAD_DIM = 128
BLOCK = 64
RANDOM = 3
GLOBAL = 128
NB_DEV = 16
CAP = 8
NBLK = 128
TOKENS = 8192
N_SEQ = 8


def query_key_pair(key):
    folded = jax.random.fold_in(key, 11)
    streams = jax.random.split(folded, 8)
    total_width = HEADS * HEAD_DIM
    row_ids = jnp.arange(TOKENS, dtype=jnp.int32)[:, None]
    query_scale = jnp.where(row_ids < GLOBAL, 3.0, 2.0)
    query_values = jax.random.normal(streams[0], (TOKENS, total_width), jnp.float32) * query_scale
    key_values = jax.random.normal(streams[1], (TOKENS, total_width), jnp.float32)
    return (jnp.clip(query_values, -8.0, 8.0), jnp.clip(key_values, -8.0, 8.0))


def draw_queries(key, part):
    return query_key_pair(key)[0].astype(jnp.bfloat16)


def draw_key_rows(key, part):
    return query_key_pair(key)[1].astype(jnp.bfloat16)


def with_ends(values, key, low, largest):
    longest = values.shape.index(max(values.shape))
    spots = []
    for shift in (0, 1):
        where = [jax.random.randint(jax.random.fold_in(key, axis), (), 0, length) for axis, length in enumerate(values.shape)]
        where[longest] = (where[longest] + shift) % values.shape[longest]
        spots.append(tuple(where))
    return values.at[spots[0]].set(low).at[spots[1]].set(largest)


def level_of(stream_key, extent, cuts, low, high):
    gain = 1.0
    for dim, shards_of in cuts:
        steps = jax.random.uniform(jax.random.fold_in(jax.random.fold_in(stream_key, 6), dim), (shards_of,), jnp.float32, low / len(cuts), high / len(cuts))
        gain = gain * jnp.repeat(jnp.exp(steps), extent[dim] // shards_of).reshape((-1,) + (1,) * (len(extent) - 1 - dim))
    return gain


def assign_block(rng, own, number, rows, amount, top, most, slope):
    order = jax.random.permutation(rng, amount)
    crowded, common = shares(amount, rows * top, most, slope, True), shares(amount, rows * top, most, slope, False)
    places = jnp.arange(amount)

    def named(tallies, turn):
        used = int((tallies > 0).sum())
        fixed = max(1, used // 4)
        passed = fixed + (places - fixed + turn * (used - fixed)) % max(1, amount - fixed)
        return jnp.zeros((amount,), jnp.int32).at[order[jnp.where(places < fixed, places, passed)]].set(jnp.asarray(tallies, jnp.int32))

    tallies = jnp.where(number % 4 == 0, named(crowded, number // 4), named(common, number - number // 4 - 1))
    mixed = jax.random.permutation(jax.random.fold_in(own, 3), amount)
    giver, taker = mixed[0:amount // 2 * 2:2], mixed[1:amount // 2 * 2:2]
    margin = jnp.minimum(tallies[giver] - 1, most - tallies[taker]) // 2
    margin = jnp.where((giver == order[0]) | (taker == order[0]) | (tallies[taker] == 0), 0, jnp.maximum(margin, 0))
    passed = jax.random.randint(jax.random.fold_in(own, 4), (amount // 2,), 0, 1 << 20) % (margin + 1)
    tallies = tallies.at[giver].add(-passed).at[taker].add(passed)
    labels = jnp.searchsorted(jnp.cumsum(tallies), jnp.arange(rows * top), side="right").astype(jnp.int32)
    listing = labels.reshape(top, rows).T
    listing = listing[jax.random.permutation(jax.random.fold_in(own, 1), rows)]
    turn = jax.random.randint(jax.random.fold_in(own, 2), (rows, 1), 0, top)
    return jnp.take_along_axis(listing, (jnp.arange(top)[None, :] + turn) % top, axis=1)


def shares(number_of, total, bound, slope, full):
    weights = [(1 << 20) // math.isqrt(grade ** slope) + 1 for grade in range(1, number_of + 1)]
    largest = bound if full else min(bound, max(-(-total // number_of), total * weights[0] // sum(weights)))
    least = 1 if total - largest >= number_of - 1 else 0
    counts, surplus = [largest] + [least] * (number_of - 1), total - largest - least * (number_of - 1)
    while surplus > 0:
        movable = [i for i in range(1, number_of) if counts[i] < largest] or [i for i in range(1, number_of) if counts[i] < bound]
        mass, budget = sum([weights[i] for i in movable]), surplus
        for i in movable:
            extra = min(bound - counts[i], max(1, budget * weights[i] // mass), surplus)
            counts[i] = counts[i] + extra
            surplus = surplus - extra
    return np.array(counts)


def noise(own_key, dims, spread, limit, cuts=(), kind=jnp.bfloat16):
    level = level_of(own_key, dims, cuts, -0.22, 0.18) if cuts else 1.0
    values = jax.random.normal(own_key, dims, jnp.float32) * spread * level
    return jnp.minimum(jnp.maximum(values, -limit), limit).astype(kind)


def setup_inputs(seed: int = 0) -> dict:
    arg_keys = jax.random.split(jax.random.key(seed), 7)
    queries = draw_queries(jax.random.fold_in(arg_keys[6], 71), 0)
    key_rows = draw_key_rows(jax.random.fold_in(arg_keys[6], 71), 0)
    value_rows = noise(arg_keys[2], (TOKENS, HEADS * HEAD_DIM), 1.0, 6.0, ((0, 8), (1, 4)))
    random_owner_keys = jax.random.split(jax.random.fold_in(arg_keys[3], 1), NBLK // NB_DEV)
    random_owner_turns = jax.random.permutation(jax.random.fold_in(arg_keys[3], 3), NBLK // NB_DEV)
    random_owner = jax.vmap(lambda own, number: assign_block(jax.random.fold_in(arg_keys[3], 2), own, number, NB_DEV, NBLK // NB_DEV, RANDOM, CAP, 2))(random_owner_keys, random_owner_turns).reshape((NBLK, RANDOM))
    random_local = with_ends(jax.random.randint(arg_keys[4], (NBLK, RANDOM), 0, NB_DEV), jax.random.fold_in(arg_keys[4], 1), 0, NB_DEV - 1).astype(jnp.int32)
    output_weight = noise(arg_keys[5], (HEADS * HEAD_DIM, D), (HEADS * HEAD_DIM) ** -0.5, 0.09375, ((0, 4),))
    return dict(queries=queries, key_rows=key_rows, value_rows=value_rows, random_owner=random_owner, random_local=random_local, output_weight=output_weight)


masked_score = -1e30


def sparse_block(block_index, queries, key_padded, value_padded, key_rows, value_rows, random_block):
    score_scale = HEAD_DIM ** -0.5
    first_row = block_index * BLOCK
    query_block = lax.dynamic_slice_in_dim(queries, first_row, BLOCK, 0)
    window_keys = lax.dynamic_slice_in_dim(key_padded, first_row, 3 * BLOCK, 0)
    window_values = lax.dynamic_slice_in_dim(value_padded, first_row, 3 * BLOCK, 0)
    picked = random_block[block_index]
    offsets = (picked[:, None] * BLOCK + jnp.arange(BLOCK, dtype=jnp.int32)[None, :]).reshape(-1).astype(jnp.int32)
    random_keys = jnp.take(key_rows, offsets, axis=0)
    random_values = jnp.take(value_rows, offsets, axis=0)
    listed_keys = jnp.concatenate([window_keys, random_keys, key_rows[:GLOBAL]], axis=0)
    listed_values = jnp.concatenate([window_values, random_values, value_rows[:GLOBAL]], axis=0)
    listed = listed_keys.shape[0]
    slot_number = jnp.arange(listed, dtype=jnp.int32) // BLOCK
    usable = jnp.logical_and(jnp.logical_or(slot_number != 0, block_index > 0), jnp.logical_or(slot_number != 2, block_index < NBLK - 1))
    query_heads = query_block.astype(jnp.float32).reshape(BLOCK, HEADS, HEAD_DIM)
    key_heads = listed_keys.astype(jnp.float32).reshape(listed, HEADS, HEAD_DIM)
    value_heads = listed_values.astype(jnp.float32).reshape(listed, HEADS, HEAD_DIM)
    scores = jnp.einsum("qhd,khd->hqk", query_heads, key_heads) * score_scale
    scores = jnp.where(usable[None, None, :], scores, masked_score)
    row_max = jnp.max(scores, axis=2, keepdims=True)
    weight = jnp.where(usable[None, None, :], jnp.exp(scores - row_max), 0.0)
    row_total = jnp.sum(weight, axis=2)
    rounded = lax.optimization_barrier(weight.astype(jnp.bfloat16)).astype(jnp.float32)
    context = jnp.einsum("hqk,khd->qhd", rounded, value_heads) / jnp.transpose(row_total)[:, :, None]
    return context.reshape(BLOCK, HEADS * HEAD_DIM).astype(jnp.bfloat16)


def segment_part(segment, global_query, key_rows, value_rows):
    segment_rows = NB_DEV * BLOCK
    score_scale = HEAD_DIM ** -0.5
    segment_keys = lax.dynamic_slice_in_dim(key_rows, segment * segment_rows, segment_rows, 0)
    segment_values = lax.dynamic_slice_in_dim(value_rows, segment * segment_rows, segment_rows, 0)
    query_heads = global_query.astype(jnp.float32).reshape(GLOBAL, HEADS, HEAD_DIM)
    key_heads = segment_keys.astype(jnp.float32).reshape(segment_rows, HEADS, HEAD_DIM)
    value_heads = segment_values.astype(jnp.float32).reshape(segment_rows, HEADS, HEAD_DIM)
    scores = jnp.einsum("qhd,khd->hqk", query_heads, key_heads) * score_scale
    row_max = jnp.max(scores, axis=2)
    weight = jnp.exp(scores - row_max[:, :, None])
    row_total = jnp.sum(weight, axis=2)
    rounded = lax.optimization_barrier(weight.astype(jnp.bfloat16)).astype(jnp.float32)
    partial_value = jnp.einsum("hqk,khd->hqd", rounded, value_heads)
    return row_max, row_total, partial_value


def reference(queries, key_rows, value_rows, random_owner, random_local, output_weight):
    random_block = (random_owner * NB_DEV + random_local).astype(jnp.int32)
    total_width = HEADS * HEAD_DIM
    zero_block = jnp.zeros((BLOCK, total_width), key_rows.dtype)
    key_padded = jnp.concatenate([zero_block, key_rows, zero_block], axis=0)
    value_padded = jnp.concatenate([zero_block, value_rows, zero_block], axis=0)

    def one_block(block_index):
        return sparse_block(block_index, queries, key_padded, value_padded, key_rows, value_rows, random_block)

    sparse = lax.map(one_block, jnp.arange(NBLK, dtype=jnp.int32)).reshape(TOKENS, total_width)
    global_query = queries[:GLOBAL]

    def one_segment(segment):
        return segment_part(segment, global_query, key_rows, value_rows)

    segment_max, segment_total, segment_acc = lax.map(one_segment, jnp.arange(N_SEQ, dtype=jnp.int32))
    overall_max = jnp.max(segment_max, axis=0)
    factor = jnp.exp(segment_max - overall_max[None])
    global_out = jnp.sum(factor[..., None] * segment_acc, axis=0) / jnp.sum(factor * segment_total, axis=0)[..., None]
    global_out = jnp.transpose(global_out, (1, 0, 2)).reshape(GLOBAL, total_width)
    attention = jnp.concatenate([global_out.astype(jnp.bfloat16), sparse[GLOBAL:]], axis=0)
    return jnp.dot(attention, output_weight, preferred_element_type=jnp.float32).astype(jnp.bfloat16)
```

```python
import functools
import math

import jax
import jax.numpy as jnp
from jax import lax
from jax.experimental import pallas as pl
from jax.experimental.pallas import tpu as pltpu
from jax.sharding import PartitionSpec as P

HEAD_DIM = 128
BLOCK = 64
RANDOM = 3
GLOBAL = 128
CHUNKS = 2
PAIR = 2


masked_score = -1e30


def slot_table(owner_ids, local_ids, seq_count, slot_count):
    owner_hits = (owner_ids[:, None] == jnp.arange(seq_count, dtype=jnp.int32)[None, :]).astype(
        jnp.int32
    )
    earlier = jnp.cumsum(owner_hits, axis=0) - owner_hits
    slot_ids = jnp.sum(earlier * owner_hits, axis=1)
    slot_hits = (slot_ids[:, None] == jnp.arange(slot_count, dtype=jnp.int32)[None, :]).astype(
        jnp.int32
    )
    request_table = jnp.sum(
        (owner_hits * local_ids[:, None])[:, :, None] * slot_hits[:, None, :], axis=0
    )
    return (request_table, slot_ids)


def attend_kernel(heads, index_ref, flag_ref, q_ref, *refs):
    near, out_ref = refs[:-1], refs[-1]
    step = pl.program_id(0)
    rate = HEAD_DIM ** (-0.5) * math.log2(math.e)
    first, last = flag_ref[0, step], flag_ref[1, step]
    listed = len(near) * BLOCK
    column = lax.broadcasted_iota(jnp.int32, (1, listed), 1) // BLOCK
    hidden = jnp.logical_or(
        jnp.logical_and(column == 0, first == 1), jnp.logical_and(column == 2, last == 1)
    )
    bias = jnp.where(hidden, masked_score, 0.0).astype(jnp.float32)
    for head in range(heads):
        here = pl.ds(head * HEAD_DIM, HEAD_DIM)
        keys = jnp.concatenate([ref[0, 0, :, here] for ref in near], axis=0)
        values = jnp.concatenate([ref[0, 1, :, here] for ref in near], axis=0)
        scores = lax.dot_general(
            q_ref[:, here], keys, (((1,), (1,)), ((), ())), preferred_element_type=jnp.float32
        )
        scores = scores + bias
        top = jnp.max(scores, axis=1, keepdims=True)
        weight = jnp.exp2((scores - top) * rate)
        total = jnp.sum(weight, axis=1, keepdims=True)
        context = jnp.dot(
            weight.astype(jnp.bfloat16), values, preferred_element_type=jnp.float32
        )
        out_ref[:, here] = (context / total).astype(out_ref.dtype)


def attend(queries, pool, index, flags):
    tokens, width = queries.shape
    blocks = tokens // BLOCK
    heads = width // HEAD_DIM
    listed = index.shape[0]

    def picked(r):
        return pl.BlockSpec(
            (1, 2, BLOCK, width), lambda i, index_ref, flag_ref: (index_ref[r, i], 0, 0, 0)
        )

    return pl.pallas_call(
        functools.partial(attend_kernel, heads),
        grid_spec=pltpu.PrefetchScalarGridSpec(
            num_scalar_prefetch=2,
            grid=(blocks,),
            in_specs=[pl.BlockSpec((BLOCK, width), lambda i, a, b: (i, 0))]
            + [picked(r) for r in range(listed)],
            out_specs=pl.BlockSpec((BLOCK, width), lambda i, a, b: (i, 0)),
        ),
        out_shape=jax.ShapeDtypeStruct(queries.shape, jnp.bfloat16),
        compiler_params=pltpu.CompilerParams(dimension_semantics=("arbitrary",)),
        cost_estimate=pl.CostEstimate(
            flops=60 * tokens * width * 8 * BLOCK,
            bytes_accessed=blocks * 14 * BLOCK * width * 2,
            transcendentals=tokens * heads * 8 * BLOCK,
        ),
    )(index, flags, queries, *([pool] * listed))


def merged(left, right):
    joint = jnp.maximum(left[0], right[0])
    a, b = jnp.exp(left[0] - joint), jnp.exp(right[0] - joint)
    return (
        joint,
        left[1] * a + right[1] * b,
        left[2] * a[:, :, None] + right[2] * b[:, :, None],
    )


def partial_softmax(query, keys, values):
    tokens, width = query.shape
    heads = width // HEAD_DIM
    query = query.reshape(tokens, heads, HEAD_DIM)
    keys, values = (a.reshape(-1, heads, HEAD_DIM) for a in (keys, values))
    scores = jnp.einsum("qhd,khd->hqk", query, keys, preferred_element_type=jnp.float32)
    scores = scores * HEAD_DIM ** (-0.5)
    row_max = jnp.max(scores, axis=2)
    weight = jnp.exp(scores - row_max[:, :, None])
    row_total = jnp.sum(weight, axis=2)
    value = jnp.einsum(
        "hqk,khd->hqd", weight.astype(jnp.bfloat16), values, preferred_element_type=jnp.float32
    )
    return row_max, row_total, value


def after(array, *others):
    return lax.optimization_barrier((array,) + others)[0]


def local(queries, key_rows, value_rows, random_owner, random_local, output_weight):
    n = lax.axis_size("seq")
    me = lax.axis_index("seq")
    heads_n = lax.axis_size("head")
    h = lax.axis_index("head")
    token_count, width_here = queries.shape
    nb = token_count // BLOCK
    gb = GLOBAL // BLOCK
    heads_here = width_here // HEAD_DIM
    slot_count = max(2, 4 * nb // n)
    depth = n // PAIR
    z, x = me // PAIR, me % PAIR

    def send(array, pairs, axis="seq"):
        return jax.tree.map(lambda part: lax.ppermute(part, axis, pairs), array)

    def swapped(array, m):
        return lax.ppermute(array, "head", [(i, i ^ m) for i in range(heads_n)])

    def folded(part, pairs, here):
        packed = jnp.concatenate([part[2], part[0][:, None], part[1][:, None]], axis=1)
        got = send(packed, pairs)
        both = merged(part, (got[:, GLOBAL], got[:, GLOBAL + 1], got[:, :GLOBAL]))
        return jax.tree.map(lambda a, b: jnp.where(here, a, b), both, part)

    def finished(part):
        out = jnp.transpose(part[2] / part[1][:, :, None], (1, 0, 2))
        return out.reshape(GLOBAL, -1).astype(jnp.bfloat16)

    chunks = math.gcd(CHUNKS, heads_here)
    cw = width_here // chunks
    cuts = [slice(c * cw, (c + 1) * cw) for c in range(chunks)]
    key_blocks = key_rows.reshape(nb, BLOCK, width_here)
    value_blocks = value_rows.reshape(nb, BLOCK, width_here)
    owned = [jnp.stack([key_blocks[..., sl], value_blocks[..., sl]], axis=1) for sl in cuts]
    up = [(i, i + 1) for i in range(n - 1)]
    down = [(i + 1, i) for i in range(n - 1)]
    mates = [(i, i + 1 if i % PAIR == 0 else i - 1) for i in range(n)]
    owner_flat = random_owner.reshape(-1)
    local_flat = random_local.reshape(-1)
    request_table, slot_ids = slot_table(owner_flat, local_flat, n, slot_count)
    line_wins = n % PAIR == 0 and nb <= PAIR * slot_count
    global_ids = jnp.arange(gb, dtype=jnp.int32)
    pools, tops, last = [], [], None

    if line_wins:
        mate_owner, mate_local = send((owner_flat, local_flat), mates)
        near_query = jnp.where(me == 1, send(queries[:GLOBAL], [(0, 1)]), queries[:GLOBAL])
        befores = [send(own[-1:], up) for own in owned]
        afters = [send(own[:1], down) for own in owned]
        mate_table, _ = slot_table(mate_owner, mate_local, n, slot_count)
        fetch = slot_count + gb
        mate_table = jnp.concatenate(
            [mate_table, jnp.broadcast_to(global_ids[None], (n, gb))], axis=1
        )
        offsets = [0]
        for s in range(1, depth):
            offsets += [-s, s]
        bufs = [{0: own} for own in owned]
        for s in range(1, depth):
            upward = [(i, i + PAIR) for i in range((s - 1) * PAIR, n - PAIR)]
            downward = [(i, i - PAIR) for i in range(PAIR, n - (s - 1) * PAIR)]
            for held in bufs:
                held[-s] = send(held[1 - s], upward)
                held[s] = send(held[s - 1], downward)
        for c in range(chunks):
            crossed = []
            for d in offsets:
                holder = jnp.clip((z + d) * PAIR + x, 0, n - 1)
                asked = jnp.take(bufs[c][d], mate_table[holder], axis=0)
                good = [(i, j) for i, j in mates if 0 <= i // PAIR + d < depth]
                crossed.append(send(asked, good))
            part = None
            for s in range(depth):
                held = bufs[c][s]
                term = partial_softmax(near_query[:, cuts[c]], held[:, 0], held[:, 1])
                part = term if part is None else merged(part, term)
            tops.append(finished(folded(part, [(1, 0)], me == 0)))
            pools.append(
                jnp.concatenate(
                    [bufs[c][d] for d in offsets] + crossed + [befores[c], afters[c]], axis=0
                )
            )
        last = bufs[0][depth - 1]
        place = jnp.where(owner_flat // PAIR < z, 2 * (z - owner_flat // PAIR) - 1,
                          2 * (owner_flat // PAIR - z))
        line_total = len(offsets) * nb
        cell = jnp.where(
            owner_flat % PAIR == x,
            place * nb + local_flat,
            line_total + place * fetch + slot_ids,
        )
        root = jnp.maximum(2 * z - 1, 0)
        global_cell = global_ids + jnp.where(
            x == 0, root * nb, line_total + root * fetch + slot_count
        )
        edge = line_total + len(offsets) * fetch
    else:
        rows = jnp.stack([queries[:GLOBAL], key_rows[:GLOBAL], value_rows[:GLOBAL]])
        rows = jnp.where(me == 1, send(rows, [(0, 1)]), rows)
        for s in range(1, depth):
            got = send(rows, [((s - 1) * PAIR + q, s * PAIR + q) for q in range(PAIR)])
            rows = jnp.where(z == s, got, rows)
        part = partial_softmax(rows[0], key_rows, value_rows)
        for s in range(depth - 1, 0, -1):
            pairs = [(s * PAIR + q, (s - 1) * PAIR + q) for q in range(PAIR)]
            part = folded(part, pairs, z == s - 1)
        top = finished(folded(part, [(1, 0)], me == 0))
        wanted = lax.all_to_all(request_table, "seq", split_axis=0, concat_axis=0, tiled=True)
        for c, own in enumerate(owned):
            tops.append(top[:, cuts[c]])
            sent = jnp.take(own, wanted.reshape(-1), axis=0)
            got = lax.all_to_all(sent, "seq", split_axis=0, concat_axis=0, tiled=True)
            shared = jnp.stack(
                [rows[i][:, cuts[c]].reshape(gb, BLOCK, cw) for i in (1, 2)], axis=1
            )
            edges = [send(own[-1:], up), send(own[:1], down)]
            pools.append(jnp.concatenate([own, got, shared] + edges, axis=0))
        cell = nb + owner_flat * slot_count + slot_ids
        global_cell = nb + n * slot_count + global_ids
        edge = nb + n * slot_count + gb

    weights, order, bit = [output_weight], [0], heads_n
    while bit > 1:
        bit //= 2
        for m in list(order):
            held = weights[order.index(m)]
            if m and last is not None:
                held = after(held, last)
            weights.append(swapped(held, bit))
            order.append(m ^ bit)

    steps = jnp.arange(nb, dtype=jnp.int32)
    cell = cell.reshape(nb, RANDOM)
    index = jnp.stack(
        [
            jnp.where(steps == 0, edge, steps - 1),
            steps,
            jnp.where(steps == nb - 1, edge + 1, steps + 1),
        ]
        + [cell[:, r] for r in range(RANDOM)]
        + [jnp.broadcast_to(global_cell[g], (nb,)) for g in range(gb)]
    ).astype(jnp.int32)
    numbers = me * nb + steps
    flags = jnp.stack([numbers == 0, numbers == n * nb - 1]).astype(jnp.int32)

    share = token_count // heads_n
    pieces = [[] for _ in order]
    for c, sl in enumerate(cuts):
        sparse = attend(queries[:, sl], pools[c], index, flags)
        top = jnp.where(me == 0, tops[c], sparse[:GLOBAL])
        sparse = jnp.concatenate([top, sparse[GLOBAL:]], axis=0)
        for k, m in enumerate(order):
            piece = lax.dynamic_slice_in_dim(sparse, (h ^ m) * share, share, 0)
            pieces[k].append(piece if m == 0 else swapped(piece, m))
    total = None
    for k in range(len(order)):
        term = jnp.dot(
            jnp.concatenate(pieces[k], axis=1), weights[k], preferred_element_type=jnp.float32
        )
        total = term if total is None else total + term
    return total.astype(jnp.bfloat16)


def solution(mesh):
    in_specs = (
        P("seq", "head"),
        P("seq", "head"),
        P("seq", "head"),
        P("seq", None),
        P("seq", None),
        P("head", None),
    )
    out_specs = P(("seq", "head"), None)
    return jax.shard_map(local, mesh=mesh, in_specs=in_specs, out_specs=out_specs, check_vma=False)
```
